32 devices in a mesh: parts: 2 (over y), brick: 4 (over z), rep: 2 (over x), sub: 2 (over core).
Axes of the slice: x: 2, y: 2, z: 4, core: 2. Of those that a mesh axis runs over, the one named last changes fastest.
Arguments:
- fine_cells: int32 [5, 32768], P(None, ('parts', 'brick', 'rep', 'sub')), parts along dimension 1, may hold values from 0 to 511, as said below
- fine_exponent: float32 [32768], P(('parts', 'brick', 'rep', 'sub')), parts along dimension 0, may hold values from 0.05 to 0.6
- fine_charge: float32 [32768], P(('parts', 'brick', 'rep', 'sub')), parts along dimension 0, may hold values from -6 to 6
- fine_offset: float32 [3, 32768], P(None, ('parts', 'brick', 'rep', 'sub')), parts along dimension 1, may hold values from 0 to 1
- wide_cells: int32 [5, 4096], P(None, ('parts', 'brick', 'rep', 'sub')), parts along dimension 1, may hold values from 0 to 127, as said below
- wide_exponent: float32 [4096], P(('parts', 'brick', 'rep', 'sub')), parts along dimension 0, may hold values from 0.05 to 0.6
- wide_charge: float32 [4096], P(('parts', 'brick', 'rep', 'sub')), parts along dimension 0, may hold values from -6 to 6
- wide_offset: float32 [3, 4096], P(None, ('parts', 'brick', 'rep', 'sub')), parts along dimension 1, may hold values from 0 to 1
Outputs:
- finest_grid: float32 [256, 512, 512], P(('parts', 'brick'), ('rep', 'sub')), parts along dimension 0
- second_grid: float32 [128, 256, 256], P(('parts', 'brick'), ('rep', 'sub')), parts along dimension 0
- middle_grid: float32 [64, 16384], P('parts', 'brick'), parts along dimension 0
- coarse_grid: float32 [32, 4096], P('parts', 'brick'), parts along dimension 0
- coarsest_grid: float32 [16, 1024], P('parts', 'brick'), parts along dimension 0
The draws below stay inside these ranges and needn't reach their ends.
There are 2 independent parts, one for each index of `parts`. The reference program is written for one: setup_inputs(seed, part) draws one part's arguments, and reference() takes and returns one part's arrays. A program takes and returns all parts, laid end to end along the dimension named above; each array names one. Nothing has to cross between parts.
Inputs may be any that keep to these rules, and one draw needn't show every extreme that they name: `fine_cells`: column n is one fine Gaussian: row 0 its level L (0 or 1), row 1 its radius (1 to 4, equal to 4 on every 16th column), rows 2 to 4 its centre cell on level L's grid. The centre lies in the block of the device that holds column n: along the first dimension within that device's brick block of 128/2^L/4 cells, along the second within its block of 512/2^L/4 cells along rep+sub, anywhere along the third. `wide_cells`: column n is one wide Gaussian: row 0 its level L (2 to 4), row 1 its radius (1 to 4, equal to 4 on every 16th column), rows 2 to 4 its centre cell, anywhere on level L's grid.
All inputs are finite; a program needn't handle non-finite values.
Results may differ from the reference program's by a relative error of at most 0.0038.
Values sent between devices are 32-bit elements; how exact they have to be, the bound alone decides.
No kernel may reach another device: no remote copies, remote signals or barrier semaphores. Data moves between devices by JAX's collectives and lax.ppermute only.
A program may use at most 64 MiB of HBM per device.

```python
import math
import jax
import jax.numpy as jnp
from jax import lax

GRID = 512
ROWS = 128
HALF = 4
FINE_DEV = 1024
WIDE_DEV = 128
FINE = 16384
WIDE = 2048
N_BRICK = 4
N_REP = 2
N_SUB = 2


def draw_fine_cells(key, part):
    slot_count = FINE_DEV * N_BRICK * N_REP * N_SUB
    slots = jnp.arange(slot_count, dtype=jnp.int32)
    device = slots // FINE_DEV
    columns = N_REP * N_SUB
    brick_index = device // columns
    column_index = device % columns
    level_row = (jax.random.randint(jax.random.fold_in(key, 1), (slot_count,), 0, 4) == 0).astype(jnp.int32)
    radius = jax.random.randint(jax.random.fold_in(key, 2), (slot_count,), 1, HALF + 1)
    radius = jnp.where(slots % 16 == 0, HALF, radius)
    row_tile = jnp.right_shift(jnp.int32(ROWS), level_row) // N_BRICK
    period = jnp.right_shift(jnp.int32(GRID), level_row)
    col_tile = period // columns
    picks = jax.random.randint(jax.random.fold_in(key, 3), (3, slot_count), 0, 1 << 20)
    first_cell = brick_index * row_tile + picks[0] % row_tile
    second_cell = column_index * col_tile + picks[1] % col_tile
    third_cell = picks[2] % period
    return jnp.stack([level_row, radius, first_cell, second_cell, third_cell]).astype(jnp.int32)


def draw_wide_cells(key, part):
    slot_count = WIDE_DEV * N_BRICK * N_REP * N_SUB
    slots = jnp.arange(slot_count, dtype=jnp.int32)
    choose = jax.random.randint(jax.random.fold_in(key, 5), (slot_count,), 0, 8)
    level_row = jnp.where(slots % 8 == 3, 4, jnp.where(choose < 2, 3, 2)).astype(jnp.int32)
    radius = jax.random.randint(jax.random.fold_in(key, 6), (slot_count,), 1, HALF + 1)
    radius = jnp.where(slots % 16 == 0, HALF, radius)
    rows_here = jnp.right_shift(jnp.int32(ROWS), level_row)
    period = jnp.right_shift(jnp.int32(GRID), level_row)
    picks = jax.random.randint(jax.random.fold_in(key, 7), (3, slot_count), 0, 1 << 20)
    first_cell = picks[0] % rows_here
    second_cell = picks[1] % period
    third_cell = picks[2] % period
    return jnp.stack([level_row, radius, first_cell, second_cell, third_cell]).astype(jnp.int32)


def block_levels(key, shape, shards, least, high):
    loudness, own = 1.0, jax.random.fold_in(key, 6)
    for axis_at, parts in shards:
        draws = jnp.exp(jax.random.uniform(jax.random.fold_in(own, axis_at), (parts,), jnp.float32, least / len(shards), high / len(shards)))
        loudness = loudness * jnp.repeat(draws, shape[axis_at] // parts).reshape([-1 if axis == axis_at else 1 for axis in range(len(shape))])
    return loudness


def bell_draw(rng, dims, scale, reach, cuts=(), kind=jnp.bfloat16):
    drawn = jax.random.normal(rng, dims, jnp.float32) * scale
    if len(cuts) > 0:
        drawn = block_levels(rng, dims, cuts, -0.22, 0.18) * drawn
    return jnp.clip(drawn, min=-reach, max=reach).astype(kind)


def setup_inputs(seed: int = 0, part: int = 0) -> dict:
    splits = jax.random.split(jax.random.key(seed), 9)
    own_keys = jax.random.split(jax.random.fold_in(splits[8], part), 9)
    return {
        "fine_cells": draw_fine_cells(jax.random.fold_in(jax.random.fold_in(splits[8], part), 71), part),
        "fine_exponent": jnp.clip(jnp.exp(math.log(0.6) - 2.4849067 * jax.random.uniform(own_keys[1], (FINE,), jnp.float32) ** block_levels(own_keys[1], (FINE,), ((0, 16),), -0.2, 0.2)), 0.05, 0.6),
        "fine_charge": bell_draw(own_keys[2], (FINE,), 1.0, 6.0, ((0, 16),), jnp.float32),
        "fine_offset": jnp.clip(1.0 * jax.random.uniform(own_keys[3], (3, FINE), jnp.float32) ** block_levels(own_keys[3], (3, FINE), ((1, 16),), -0.2, 0.2), 0.0, 1.0),
        "wide_cells": draw_wide_cells(jax.random.fold_in(jax.random.fold_in(splits[8], part), 71), part),
        "wide_exponent": jnp.clip(jnp.exp(math.log(0.6) - 2.4849067 * jax.random.uniform(own_keys[5], (WIDE,), jnp.float32) ** block_levels(own_keys[5], (WIDE,), ((0, 16),), -0.2, 0.2)), 0.05, 0.6),
        "wide_charge": bell_draw(own_keys[6], (WIDE,), 1.0, 6.0, ((0, 16),), jnp.float32),
        "wide_offset": jnp.clip(1.0 * jax.random.uniform(own_keys[7], (3, WIDE), jnp.float32) ** block_levels(own_keys[7], (3, WIDE), ((1, 16),), -0.2, 0.2), 0.0, 1.0),
    }


def one_factor(offsets, radius, exponent, centre_shift):
    inside = jnp.abs(offsets) <= radius[:, None]
    spread = offsets.astype(exponent.dtype) - centre_shift[:, None]
    return jnp.where(inside, jnp.exp(-exponent[:, None] * spread * spread), 0.0)


def deposit(slot_table, exponent, charge, offset, first_level, level_count):
    base_list = []
    grid_cells = 0
    for level_index in range(first_level, first_level + level_count):
        base_list.append(grid_cells)
        grid_cells += (ROWS >> level_index) * (GRID >> level_index) ** 2
    base_table = jnp.array(base_list, dtype=jnp.int32)
    slot_count = slot_table.shape[1]
    batch_size = math.gcd(slot_count, 4096)
    span_cells = jnp.arange(-HALF, HALF + 1, dtype=jnp.int32)
    span_count = 2 * HALF + 1

    def add_batch(flat_grid, batch_index):
        first_slot = (batch_index * batch_size).astype(jnp.int32)
        part_table = lax.dynamic_slice_in_dim(slot_table, first_slot, batch_size, 1)
        part_exponent = lax.dynamic_slice_in_dim(exponent, first_slot, batch_size, 0)
        part_charge = lax.dynamic_slice_in_dim(charge, first_slot, batch_size, 0)
        part_offset = lax.dynamic_slice_in_dim(offset, first_slot, batch_size, 1)
        level_row = part_table[0]
        radius = part_table[1]
        rows_here = jnp.right_shift(jnp.int32(ROWS), level_row)
        period = jnp.right_shift(jnp.int32(GRID), level_row)
        base_cell = base_table[level_row - first_level]
        offsets = jnp.broadcast_to(span_cells[None, :], (batch_size, span_count))
        row_place = part_table[2][:, None] + span_cells[None, :]
        col_place = jnp.mod(part_table[3][:, None] + span_cells[None, :], period[:, None])
        depth_place = jnp.mod(part_table[4][:, None] + span_cells[None, :], period[:, None])
        row_factor = one_factor(offsets, radius, part_exponent, part_offset[0])
        col_factor = one_factor(offsets, radius, part_exponent, part_offset[1])
        depth_factor = one_factor(offsets, radius, part_exponent, part_offset[2])
        plane_weight = ((part_charge[:, None] * row_factor)[:, :, None] * col_factor[:, None, :]).astype(jnp.bfloat16)
        depth_weight = depth_factor.astype(jnp.bfloat16)
        values = plane_weight.astype(jnp.float32)[:, :, :, None] * depth_weight.astype(jnp.float32)[:, None, None, :]
        period_four = period[:, None, None, None]
        flat_index = base_cell[:, None, None, None] + (row_place[:, :, None, None] * period_four + col_place[:, None, :, None]) * period_four + depth_place[:, None, None, :]
        inside_window = (row_place >= 0) & (row_place < rows_here[:, None])
        flat_index = jnp.where(inside_window[:, :, None, None], flat_index, grid_cells).astype(jnp.int32)
        flat_grid = flat_grid.at[flat_index.reshape(-1)].add(values.reshape(-1), mode="drop")
        return flat_grid, None

    start_grid = jnp.zeros((grid_cells,), jnp.float32)
    flat_grid, unused = lax.scan(add_batch, start_grid, jnp.arange(slot_count // batch_size, dtype=jnp.int32))
    return flat_grid


def reference(fine_cells, fine_exponent, fine_charge, fine_offset, wide_cells, wide_exponent, wide_charge, wide_offset):
    fine_flat = deposit(fine_cells, fine_exponent, fine_charge, fine_offset, 0, 2)
    level_zero = ROWS * GRID * GRID
    finest_grid = fine_flat[:level_zero].reshape(ROWS, GRID, GRID)
    second_grid = fine_flat[level_zero:].reshape(ROWS // 2, GRID // 2, GRID // 2)
    wide_flat = deposit(wide_cells, wide_exponent, wide_charge, wide_offset, 2, 3)
    outputs = []
    first_cell = 0
    for level_index in range(2, 5):
        rows_here = ROWS >> level_index
        period = GRID >> level_index
        outputs.append(wide_flat[first_cell:first_cell + rows_here * period * period].reshape(rows_here, period * period))
        first_cell += rows_here * period * period
    return (finest_grid, second_grid, outputs[0], outputs[1], outputs[2])
```

```python
import math

import jax
import jax.numpy as jnp
from jax import lax
from jax.experimental import pallas as pl
from jax.experimental.pallas import tpu as pltpu
from jax.sharding import PartitionSpec as P

GRID = 512
ROWS = 128
HALF = 4
SIDE = 8
COLUMNS = ("rep", "sub")
LEVEL, RADIUS, CENTRE, SHIFT, EXPONENT, CHARGE = 0, 1, 2, 5, 8, 9


def pack(cells, exponent, charge, offset):
    return jnp.concatenate(
        [cells.astype(jnp.float32), offset, exponent[None, :], charge[None, :]], 0
    )


def shifted(array, axis, by, wrap):
    devices = lax.axis_size(axis)
    pairs = [(i, (i + by) % devices) for i in range(devices) if wrap or 0 <= i + by < devices]
    return lax.ppermute(array, axis, pairs)


def window(first, count, table, dim, period):
    radius = table(RADIUS)
    span = radius.astype(jnp.int32)
    start = table(CENTRE + dim).astype(jnp.int32) - span - first
    cells = lax.broadcasted_iota(jnp.int32, (count, radius.shape[1]), 0)
    step = cells - start
    if period is not None:
        step = step & (period - 1)
        inside = step <= 2 * span
    else:
        inside = (step >= 0) & (step <= 2 * span)
    spread = step.astype(jnp.float32) - (radius + table(SHIFT + dim))
    return jnp.where(inside, jnp.exp((-table(EXPONENT)) * spread * spread), 0.0)


def row_window(first, count, table, level):
    charge = jnp.where(table(LEVEL) == float(level), table(CHARGE), 0.0)
    return charge * window(first, count, table, 0, None)


def fill_depth(depth, read, slots, period):
    lanes = math.gcd(slots, 256)
    piece = math.gcd(period, 32)
    for lane in range(0, slots, lanes):
        table = read(lane, lanes)

        def body(at, carry, table=table, lane=lane):
            first = pl.multiple_of(at * piece, piece)
            depth[pl.ds(first, piece), lane : lane + lanes] = window(
                first, piece, table, 2, period
            ).astype(jnp.bfloat16)
            return carry

        lax.fori_loop(0, period // piece, body, 0, unroll=2)


def product(lhs, depth):
    return lax.dot_general(
        lhs, depth, (((1,), (1,)), ((), ())), preferred_element_type=jnp.float32
    )


def fine_kernel(level, row_tile, col_tile, period, slots):
    steps = row_tile // HALF

    def kernel(place, below, here, above, out, depth, near, cols, lhs, side):
        at = pl.program_id(0)
        first_row = place[0] * row_tile
        first_col = place[1] * col_tile

        def reader(ref, block):
            def read(lane, lanes):
                return lambda row: ref[block, row : row + 1, lane : lane + lanes]

            return read

        def whole(ref, block):
            return lambda row: ref[block, row : row + 1, :]

        def plane(row_values, rows, col_ref, col_count):
            for r in range(rows):
                for c in range(0, col_count, 16):
                    lhs[r * col_count + c : r * col_count + c + 16, :] = (
                        row_values[r : r + 1, :] * col_ref[c : c + 16, :]
                    ).astype(jnp.bfloat16)
            return lhs[0 : rows * col_count, :]

        def narrow(row_values, rows, col_values):
            for r in range(0, rows, 2):
                lhs[r * SIDE : (r + 2) * SIDE, :] = jnp.concatenate(
                    [row_values[r : r + 1, :] * col_values, row_values[r + 1 : r + 2, :] * col_values],
                    0,
                ).astype(jnp.bfloat16)
            return lhs[0 : rows * SIDE, :]

        def fill_cols(ref, block):
            def body(j, carry):
                first = pl.multiple_of(j * 16, 16)
                cols[pl.ds(first, 16), :] = window(
                    first_col + first, 16, whole(ref, block), 1, period
                )
                return carry

            lax.fori_loop(0, col_tile // 16, body, 0)

        @pl.when(at == 0)
        def _():
            for k, (block, col) in enumerate(((0, 0), (2, col_tile - SIDE))):
                for ref, row, rows in (
                    (here, 0, row_tile),
                    (below, 0, HALF),
                    (above, row_tile - HALF, HALF),
                ):
                    fill_depth(near, reader(ref, block), slots, period)
                    table = whole(ref, block)
                    col_values = window(first_col + col, SIDE, table, 1, period)
                    row_values = row_window(first_row + row, max(rows, 8), table, level)
                    part = product(narrow(row_values, rows, col_values), near[...])
                    part = part.reshape(rows, SIDE, period)
                    if ref is here:
                        side[k] = part
                    else:
                        side[k, row : row + rows] += part
            fill_depth(depth, reader(here, 1), slots, period)

        def edge(ref, row):
            fill_depth(near, reader(ref, 1), slots, period)
            fill_cols(ref, 1)
            row_values = row_window(first_row + row, 8, whole(ref, 1), level)
            part = product(plane(row_values, HALF, cols, col_tile), near[...])
            out[...] += part.reshape(HALF, col_tile, period)

        def own():
            row_values = row_window(first_row + at * HALF, 8, whole(here, 1), level)
            part = product(plane(row_values, HALF, cols, col_tile), depth[...])
            out[...] = part.reshape(HALF, col_tile, period)
            rows = pl.ds(at * HALF, HALF)
            out[:, 0:SIDE, :] += side[0, rows]
            out[:, col_tile - SIDE : col_tile, :] += side[1, rows]

        @pl.when(at == 0)
        def _():
            fill_cols(here, 1)

        own()

        @pl.when(at == 0)
        def _():
            edge(below, 0)
            fill_cols(here, 1)

        @pl.when(at == steps - 1)
        def _():
            edge(above, row_tile - HALF)

    return kernel


def fine_level(level, place, below, here, above):
    row_tile = (ROWS >> level) // lax.axis_size("brick")
    period = GRID >> level
    col_tile = period // lax.axis_size(COLUMNS)
    slots = here.shape[2]
    table_spec = pl.BlockSpec(here.shape, lambda i: (0, 0, 0))
    return pl.pallas_call(
        fine_kernel(level, row_tile, col_tile, period, slots),
        name=f"fine_{level}",
        grid=(row_tile // HALF,),
        in_specs=[pl.BlockSpec(memory_space=pltpu.SMEM), table_spec, table_spec, table_spec],
        out_specs=pl.BlockSpec((HALF, col_tile, period), lambda i: (i, 0, 0)),
        out_shape=jax.ShapeDtypeStruct((row_tile, col_tile, period), jnp.float32),
        scratch_shapes=[
            pltpu.VMEM((period, slots), jnp.bfloat16),
            pltpu.VMEM((period, slots), jnp.bfloat16),
            pltpu.VMEM((col_tile, slots), jnp.float32),
            pltpu.VMEM((max(HALF * col_tile, row_tile * SIDE), slots), jnp.bfloat16),
            pltpu.VMEM((2, row_tile, SIDE, period), jnp.float32),
        ],
        compiler_params=pltpu.CompilerParams(dimension_semantics=("arbitrary",)),
    )(place, below, here, above)


def wide_levels(place, table):
    bricks = lax.axis_size("brick")
    slots = table.shape[1]
    chunk = math.gcd(slots, 1024)
    shapes = []
    for level in range(2, 5):
        period = GRID >> level
        shapes.append((ROWS >> level, period // bricks, period))

    def kernel(place, values, *refs):
        outs, (depth, lhs) = refs[:3], refs[3:]

        @pl.when(pl.program_id(0) == 0)
        def _():
            for out in outs:
                out[...] = jnp.zeros(out.shape, jnp.float32)

        def whole(row):
            return values[row : row + 1, :]

        def read(lane, lanes):
            return lambda row: values[row : row + 1, lane : lane + lanes]

        for level, (rows, cols, period), out in zip(range(2, 5), shapes, outs):
            fill_depth(depth, read, chunk, period)
            row_values = row_window(0, rows, whole, level)
            col_values = window(place[0] * cols, max(cols, 8), whole, 1, period)
            for c in range(cols):
                lhs[c * rows : (c + 1) * rows, :] = (
                    row_values * col_values[c : c + 1, :]
                ).astype(jnp.bfloat16)
            part = product(lhs[0 : cols * rows, :], depth[0:period, :])
            for c in range(cols):
                out[:, c * period : (c + 1) * period] += part[c * rows : (c + 1) * rows, :]

    return pl.pallas_call(
        kernel,
        name="wide",
        grid=(slots // chunk,),
        in_specs=[
            pl.BlockSpec(memory_space=pltpu.SMEM),
            pl.BlockSpec((table.shape[0], chunk), lambda i: (0, i)),
        ],
        out_specs=[pl.BlockSpec((r, c * p), lambda i: (0, 0)) for r, c, p in shapes],
        out_shape=[jax.ShapeDtypeStruct((r, c * p), jnp.float32) for r, c, p in shapes],
        scratch_shapes=[
            pltpu.VMEM((GRID >> 2, chunk), jnp.bfloat16),
            pltpu.VMEM((shapes[0][0] * shapes[0][1], chunk), jnp.bfloat16),
        ],
        compiler_params=pltpu.CompilerParams(dimension_semantics=("arbitrary",)),
    )(place, table)


def per_device(
    fine_cells,
    fine_exponent,
    fine_charge,
    fine_offset,
    wide_cells,
    wide_exponent,
    wide_charge,
    wide_offset,
):
    place = jnp.stack([lax.axis_index("brick"), lax.axis_index(COLUMNS)]).astype(jnp.int32)
    mine = pack(fine_cells, fine_exponent, fine_charge, fine_offset)
    here = jnp.stack(
        [shifted(mine, COLUMNS, 1, True), mine, shifted(mine, COLUMNS, -1, True)]
    )
    below = shifted(here, "brick", 1, False)
    above = shifted(here, "brick", -1, False)
    wide = lax.all_gather(
        pack(wide_cells, wide_exponent, wide_charge, wide_offset),
        ("brick",) + COLUMNS,
        axis=1,
        tiled=True,
    )
    coarse = wide_levels(place, wide)
    first = fine_level(0, place, below, here, above)
    second = fine_level(1, place, below, here, above)
    return (first, second, coarse[0], coarse[1], coarse[2])


def solution(mesh):
    slots = ("parts", "brick", "rep", "sub")
    return jax.shard_map(
        per_device,
        mesh=mesh,
        in_specs=(
            P(None, slots),
            P(slots),
            P(slots),
            P(None, slots),
            P(None, slots),
            P(slots),
            P(slots),
            P(None, slots),
        ),
        out_specs=(
            P(("parts", "brick"), COLUMNS, None),
            P(("parts", "brick"), COLUMNS, None),
            P("parts", "brick"),
            P("parts", "brick"),
            P("parts", "brick"),
        ),
        check_vma=False,
    )
```

```python
import math

import jax
import jax.numpy as jnp
from jax import lax
from jax.experimental import pallas as pl
from jax.experimental.pallas import tpu as pltpu
from jax.sharding import PartitionSpec as P

GRID = 512
ROWS = 128
HALF = 4
SIDE = 8
COLUMNS = ("rep", "sub")
LEVEL, RADIUS, CENTRE, SHIFT, EXPONENT, CHARGE = 0, 1, 2, 5, 8, 9


def pack(cells, exponent, charge, offset):
    return jnp.concatenate(
        [cells.astype(jnp.float32), offset, exponent[None, :], charge[None, :]], 0
    )


def shifted(array, axis, by, wrap):
    devices = lax.axis_size(axis)
    pairs = [(i, (i + by) % devices) for i in range(devices) if wrap or 0 <= i + by < devices]
    return lax.ppermute(array, axis, pairs)


def gathered(array, axis):
    devices, width, have = lax.axis_size(axis), array.shape[1], 1
    while have < devices:
        take = min(have, devices - have)
        array = jnp.concatenate([array, shifted(array[:, : take * width], axis, have, True)], 1)
        have += take
    return array


def window(first, count, table, dim, period):
    radius = table(RADIUS)
    span = radius.astype(jnp.int32)
    start = table(CENTRE + dim).astype(jnp.int32) - span - first
    cells = lax.broadcasted_iota(jnp.int32, (count, radius.shape[1]), 0)
    step = cells - start
    if period is not None:
        step = step & (period - 1)
        inside = step <= 2 * span
    else:
        inside = (step >= 0) & (step <= 2 * span)
    spread = step.astype(jnp.float32) - (radius + table(SHIFT + dim))
    return jnp.where(inside, jnp.exp((-table(EXPONENT)) * spread * spread), 0.0)


def row_window(first, count, table, level):
    charge = jnp.where(table(LEVEL) == float(level), table(CHARGE), 0.0)
    return charge * window(first, count, table, 0, None)


def fill_depth(depth, read, slots, cells):
    lanes = math.gcd(slots, 256)
    piece = math.gcd(cells, 32)
    tall = (8, lanes)
    for lane in range(0, slots, lanes):
        table = read(lane, lanes)
        radius = table(RADIUS)
        span = radius.astype(jnp.int32)
        start = table(CENTRE + 2).astype(jnp.int32) - span
        base = lax.broadcasted_iota(jnp.int32, tall, 0) - start
        mask = jnp.broadcast_to(jnp.right_shift(GRID, table(LEVEL).astype(jnp.int32)) - 1, tall)
        width = jnp.broadcast_to(2 * span, tall)
        centre = jnp.broadcast_to(radius + table(SHIFT + 2), tall)
        decay = jnp.broadcast_to(-table(EXPONENT), tall)

        def body(at, carry, lane=lane, base=base, mask=mask, width=width, centre=centre, decay=decay):
            first = pl.multiple_of(at * piece, piece)
            for row in range(0, piece, 16):
                halves = []
                for half in range(0, 16, 8):
                    step = (base + (first + row + half)) & mask
                    spread = step.astype(jnp.float32) - centre
                    value = jnp.exp(decay * spread * spread)
                    halves.append(jnp.where(step <= width, value, 0.0))
                depth[pl.ds(first + row, 16), lane : lane + lanes] = jnp.concatenate(
                    halves, 0
                ).astype(jnp.bfloat16)
            return carry

        lax.fori_loop(0, cells // piece, body, 0, unroll=2)


def product(lhs, depth):
    return lax.dot_general(
        lhs, depth, (((1,), (1,)), ((), ())), preferred_element_type=jnp.float32
    )


def fine_kernel(sizes, slots):
    steps = sizes[0][0] // HALF

    def kernel(place, below, here, above, out, second, depth, near, cols, near_cols, lhs, side):
        at = pl.program_id(0)

        def reader(ref, block):
            def read(lane, lanes):
                return lambda row: ref[block, row : row + 1, lane : lane + lanes]

            return read

        def whole(ref, block):
            return lambda row: ref[block, row : row + 1, :]

        def row_values(ref, block, level, row, rows):
            first = place[0] * sizes[level][0] + row
            return row_window(first, max(rows, 8), whole(ref, block), level)

        def plane(values, rows, col_ref, col_count):
            for r in range(rows):
                for c in range(0, col_count, 16):
                    lhs[r * col_count + c : r * col_count + c + 16, :] = (
                        values[r : r + 1, :] * col_ref[c : c + 16, :]
                    ).astype(jnp.bfloat16)
            return lhs[0 : rows * col_count, :]

        def narrow(values, rows, col_values):
            for r in range(0, rows, 2):
                lhs[r * SIDE : (r + 2) * SIDE, :] = jnp.concatenate(
                    [values[r : r + 1, :] * col_values, values[r + 1 : r + 2, :] * col_values], 0
                ).astype(jnp.bfloat16)
            return lhs[0 : rows * SIDE, :]

        def fill_cols(target, ref, level):
            _, col_tile, period = sizes[level]

            def body(j, carry):
                first = pl.multiple_of(j * 16, 16)
                target[pl.ds(first, 16), :] = window(
                    place[1] * col_tile + first, 16, whole(ref, 1), 1, period
                )
                return carry

            lax.fori_loop(0, col_tile // 16, body, 0)

        def middle(ref, level, row, rows, col_ref, depth_ref):
            _, col_tile, period = sizes[level]
            values = row_values(ref, 1, level, row, rows)
            part = product(plane(values, rows, col_ref, col_tile), depth_ref[0:period, :])
            return part.reshape(rows, col_tile, period)

        def rim(ref, block, level, row, rows, col):
            _, col_tile, period = sizes[level]
            col_values = window(place[1] * col_tile + col, SIDE, whole(ref, block), 1, period)
            values = row_values(ref, block, level, row, rows)
            part = product(narrow(values, rows, col_values), near[0:period, :])
            return part.reshape(rows, SIDE, period)

        @pl.when(at == 0)
        def _():
            fill_depth(depth, reader(here, 1), slots, GRID)
            fill_cols(near_cols, here, 1)
            fill_cols(cols, here, 0)
            second[...] = middle(here, 1, 0, sizes[1][0], near_cols, depth)
            for k, block in enumerate((0, 2)):
                for ref in (here, below, above):
                    fill_depth(near, reader(ref, block), slots, GRID)
                    for level in (0, 1):
                        row_tile, col_tile, _ = sizes[level]
                        col = 0 if k == 0 else col_tile - SIDE
                        rows = row_tile if ref is here else HALF
                        row = row_tile - HALF if ref is above else 0
                        part = rim(ref, block, level, row, rows, col)
                        if level == 1:
                            second[row : row + rows, col : col + SIDE, :] += part
                        elif ref is here:
                            side[k] = part
                        else:
                            side[k, row : row + rows] += part

        part = middle(here, 0, at * HALF, HALF, cols, depth)
        out[...] = part
        col_tile = sizes[0][1]
        rows = pl.ds(at * HALF, HALF)
        out[:, 0:SIDE, :] += side[0, rows]
        out[:, col_tile - SIDE : col_tile, :] += side[1, rows]

        def edge(ref, top):
            fill_depth(near, reader(ref, 1), slots, GRID)
            for level in (0, 1):
                row = sizes[level][0] - HALF if top else 0
                fill_cols(near_cols, ref, level)
                part = middle(ref, level, row, HALF, near_cols, near)
                if level == 0:
                    out[...] += part
                else:
                    second[row : row + HALF] += part

        @pl.when(at == 0)
        def _():
            edge(below, False)

        @pl.when(at == steps - 1)
        def _():
            edge(above, True)

    return kernel


def fine_levels(place, below, here, above):
    sizes = []
    for level in range(2):
        period = GRID >> level
        sizes.append(
            (
                (ROWS >> level) // lax.axis_size("brick"),
                period // lax.axis_size(COLUMNS),
                period,
            )
        )
    slots = here.shape[2]
    planes = max(HALF * sizes[0][1], sizes[0][0] * SIDE, sizes[1][0] * sizes[1][1])
    table_spec = pl.BlockSpec(here.shape, lambda i: (0, 0, 0))
    return pl.pallas_call(
        fine_kernel(sizes, slots),
        name="fine",
        grid=(sizes[0][0] // HALF,),
        in_specs=[pl.BlockSpec(memory_space=pltpu.SMEM), table_spec, table_spec, table_spec],
        out_specs=[
            pl.BlockSpec((HALF,) + sizes[0][1:], lambda i: (i, 0, 0)),
            pl.BlockSpec(sizes[1], lambda i: (0, 0, 0)),
        ],
        out_shape=[jax.ShapeDtypeStruct(size, jnp.float32) for size in sizes],
        scratch_shapes=[
            pltpu.VMEM((GRID, slots), jnp.bfloat16),
            pltpu.VMEM((GRID, slots), jnp.bfloat16),
            pltpu.VMEM((sizes[0][1], slots), jnp.float32),
            pltpu.VMEM((sizes[0][1], slots), jnp.float32),
            pltpu.VMEM((planes, slots), jnp.bfloat16),
            pltpu.VMEM((2, sizes[0][0], SIDE, GRID), jnp.float32),
        ],
        compiler_params=pltpu.CompilerParams(dimension_semantics=("arbitrary",)),
    )(place, below, here, above)


def wide_levels(place, table):
    bricks = lax.axis_size("brick")
    slots = table.shape[1]
    chunk = math.gcd(slots, 1024)
    shapes = []
    for level in range(2, 5):
        period = GRID >> level
        shapes.append((ROWS >> level, period // bricks, period))

    def kernel(place, values, *refs):
        outs, (depth, lhs) = refs[:3], refs[3:]

        @pl.when(pl.program_id(0) == 0)
        def _():
            for out in outs:
                out[...] = jnp.zeros(out.shape, jnp.float32)

        def whole(row):
            return values[row : row + 1, :]

        def read(lane, lanes):
            return lambda row: values[row : row + 1, lane : lane + lanes]

        fill_depth(depth, read, chunk, GRID >> 2)
        for level, (rows, cols, period), out in zip(range(2, 5), shapes, outs):
            row_values = row_window(0, rows, whole, level)
            col_values = window(place[0] * cols, max(cols, 8), whole, 1, period)
            for c in range(cols):
                lhs[c * rows : (c + 1) * rows, :] = (
                    row_values * col_values[c : c + 1, :]
                ).astype(jnp.bfloat16)
            part = product(lhs[0 : cols * rows, :], depth[0:period, :])
            for c in range(cols):
                out[:, c * period : (c + 1) * period] += part[c * rows : (c + 1) * rows, :]

    return pl.pallas_call(
        kernel,
        name="wide",
        grid=(slots // chunk,),
        in_specs=[
            pl.BlockSpec(memory_space=pltpu.SMEM),
            pl.BlockSpec((table.shape[0], chunk), lambda i: (0, i)),
        ],
        out_specs=[pl.BlockSpec((r, c * p), lambda i: (0, 0)) for r, c, p in shapes],
        out_shape=[jax.ShapeDtypeStruct((r, c * p), jnp.float32) for r, c, p in shapes],
        scratch_shapes=[
            pltpu.VMEM((GRID >> 2, chunk), jnp.bfloat16),
            pltpu.VMEM((shapes[0][0] * shapes[0][1], chunk), jnp.bfloat16),
        ],
        compiler_params=pltpu.CompilerParams(dimension_semantics=("arbitrary",)),
    )(place, table)


def per_device(
    fine_cells,
    fine_exponent,
    fine_charge,
    fine_offset,
    wide_cells,
    wide_exponent,
    wide_charge,
    wide_offset,
):
    place = jnp.stack([lax.axis_index("brick"), lax.axis_index(COLUMNS)]).astype(jnp.int32)
    mine = pack(fine_cells, fine_exponent, fine_charge, fine_offset)
    here = jnp.stack(
        [shifted(mine, COLUMNS, 1, True), mine, shifted(mine, COLUMNS, -1, True)]
    )
    below = shifted(here, "brick", 1, False)
    above = shifted(here, "brick", -1, False)
    wide = pack(wide_cells, wide_exponent, wide_charge, wide_offset)
    wide = gathered(gathered(wide, COLUMNS), "brick")
    coarse = wide_levels(place, wide)
    first, second = fine_levels(place, below, here, above)
    return (first, second, coarse[0], coarse[1], coarse[2])


def solution(mesh):
    slots = ("parts", "brick", "rep", "sub")
    return jax.shard_map(
        per_device,
        mesh=mesh,
        in_specs=(
            P(None, slots),
            P(slots),
            P(slots),
            P(None, slots),
            P(None, slots),
            P(slots),
            P(slots),
            P(None, slots),
        ),
        out_specs=(
            P(("parts", "brick"), COLUMNS, None),
            P(("parts", "brick"), COLUMNS, None),
            P("parts", "brick"),
            P("parts", "brick"),
            P("parts", "brick"),
        ),
        check_vma=False,
    )
```

```python
import math

import jax
import jax.numpy as jnp
from jax import lax
from jax.experimental import pallas as pl
from jax.experimental.pallas import tpu as pltpu
from jax.sharding import PartitionSpec as P

GRID = 512
ROWS = 128
HALF = 4
SIDE = 8
COLUMNS = ("rep", "sub")
LEVEL, RADIUS, CENTRE, SHIFT, EXPONENT, CHARGE = 0, 1, 2, 5, 8, 9


def pack(cells, exponent, charge, offset):
    return jnp.concatenate(
        [cells.astype(jnp.float32), offset, exponent[None, :], charge[None, :]], 0
    )


def shifted(array, axis, by):
    devices = lax.axis_size(axis)
    return lax.ppermute(array, axis, [(i, (i + by) % devices) for i in range(devices)])


def window(first, count, table, dim, period):
    radius = table(RADIUS)
    span = radius.astype(jnp.int32)
    start = table(CENTRE + dim).astype(jnp.int32) - span - first
    cells = lax.broadcasted_iota(jnp.int32, (count, radius.shape[1]), 0)
    step = cells - start
    if period is not None:
        step = step & (period - 1)
        inside = step <= 2 * span
    else:
        inside = (step >= 0) & (step <= 2 * span)
    spread = step.astype(jnp.float32) - (radius + table(SHIFT + dim))
    return jnp.where(inside, jnp.exp((-table(EXPONENT)) * spread * spread), 0.0)


def row_window(first, count, table, level):
    charge = jnp.where(table(LEVEL) == float(level), table(CHARGE), 0.0)
    return charge * window(first, count, table, 0, None)


def fill_depth(depth, read, slots, cells):
    lanes = math.gcd(slots, 256)
    piece = math.gcd(cells, 32)
    tall = (8, lanes)
    for lane in range(0, slots, lanes):
        table = read(lane, lanes)
        radius = table(RADIUS)
        span = radius.astype(jnp.int32)
        start = table(CENTRE + 2).astype(jnp.int32) - span
        base = lax.broadcasted_iota(jnp.int32, tall, 0) - start
        mask = jnp.broadcast_to(jnp.right_shift(GRID, table(LEVEL).astype(jnp.int32)) - 1, tall)
        width = jnp.broadcast_to(2 * span, tall)
        centre = jnp.broadcast_to(radius + table(SHIFT + 2), tall)
        decay = jnp.broadcast_to(-table(EXPONENT), tall)

        def body(at, carry, lane=lane, base=base, mask=mask, width=width, centre=centre, decay=decay):
            first = pl.multiple_of(at * piece, piece)
            for row in range(0, piece, 16):
                halves = []
                for half in range(0, 16, 8):
                    step = (base + (first + row + half)) & mask
                    spread = step.astype(jnp.float32) - centre
                    value = jnp.exp(decay * spread * spread)
                    halves.append(jnp.where(step <= width, value, 0.0))
                depth[pl.ds(first + row, 16), lane : lane + lanes] = jnp.concatenate(
                    halves, 0
                ).astype(jnp.bfloat16)
            return carry

        lax.fori_loop(0, cells // piece, body, 0, unroll=2)


def product(lhs, depth):
    return lax.dot_general(
        lhs, depth, (((1,), (1,)), ((), ())), preferred_element_type=jnp.float32
    )


def fine_kernel(sizes, slots, stride):
    steps = sizes[0][0] // HALF

    def kernel(place, below, here, above, out, second, depth, near, cols, near_cols, lhs, side):
        at = pl.program_id(0)

        def reader(ref, block):
            def read(lane, lanes):
                first = block * stride + lane
                return lambda row: ref[row : row + 1, first : first + lanes]

            return read

        def whole(ref, block):
            return lambda row: ref[row : row + 1, block * stride : block * stride + slots]

        def row_values(ref, block, level, row, rows):
            first = place[0] * sizes[level][0] + row
            return row_window(first, max(rows, 8), whole(ref, block), level)

        def plane(values, rows, col_ref, col_count):
            for r in range(rows):
                for c in range(0, col_count, 16):
                    lhs[r * col_count + c : r * col_count + c + 16, :] = (
                        values[r : r + 1, :] * col_ref[c : c + 16, :]
                    ).astype(jnp.bfloat16)
            return lhs[0 : rows * col_count, :]

        def narrow(values, rows, col_values):
            for r in range(0, rows, 2):
                lhs[r * SIDE : (r + 2) * SIDE, :] = jnp.concatenate(
                    [values[r : r + 1, :] * col_values, values[r + 1 : r + 2, :] * col_values], 0
                ).astype(jnp.bfloat16)
            return lhs[0 : rows * SIDE, :]

        def fill_cols(target, ref, level):
            _, col_tile, period = sizes[level]

            def body(j, carry):
                first = pl.multiple_of(j * 16, 16)
                target[pl.ds(first, 16), :] = window(
                    place[1] * col_tile + first, 16, whole(ref, 1), 1, period
                )
                return carry

            lax.fori_loop(0, col_tile // 16, body, 0)

        def middle(ref, level, row, rows, col_ref, depth_ref):
            _, col_tile, period = sizes[level]
            values = row_values(ref, 1, level, row, rows)
            part = product(plane(values, rows, col_ref, col_tile), depth_ref[0:period, :])
            return part.reshape(rows, col_tile, period)

        def rim(ref, block, level, row, rows, col):
            _, col_tile, period = sizes[level]
            col_values = window(place[1] * col_tile + col, SIDE, whole(ref, block), 1, period)
            values = row_values(ref, block, level, row, rows)
            part = product(narrow(values, rows, col_values), near[0:period, :])
            return part.reshape(rows, SIDE, period)

        @pl.when(at == 0)
        def _():
            fill_depth(depth, reader(here, 1), slots, GRID)
            fill_cols(near_cols, here, 1)
            fill_cols(cols, here, 0)
            second[...] = middle(here, 1, 0, sizes[1][0], near_cols, depth)
            for k, block in enumerate((0, 2)):
                for ref in (here, below, above):
                    fill_depth(near, reader(ref, block), slots, GRID)
                    for level in (0, 1):
                        row_tile, col_tile, _ = sizes[level]
                        col = 0 if k == 0 else col_tile - SIDE
                        rows = row_tile if ref is here else HALF
                        row = row_tile - HALF if ref is above else 0
                        part = rim(ref, block, level, row, rows, col)
                        if level == 1:
                            second[row : row + rows, col : col + SIDE, :] += part
                        elif ref is here:
                            side[k] = part
                        else:
                            side[k, row : row + rows] += part

        part = middle(here, 0, at * HALF, HALF, cols, depth)
        out[...] = part
        col_tile = sizes[0][1]
        rows = pl.ds(at * HALF, HALF)
        out[:, 0:SIDE, :] += side[0, rows]
        out[:, col_tile - SIDE : col_tile, :] += side[1, rows]

        def edge(ref, top):
            fill_depth(near, reader(ref, 1), slots, GRID)
            for level in (0, 1):
                row = sizes[level][0] - HALF if top else 0
                fill_cols(near_cols, ref, level)
                part = middle(ref, level, row, HALF, near_cols, near)
                if level == 0:
                    out[...] += part
                else:
                    second[row : row + HALF] += part

        @pl.when(at == 0)
        def _():
            edge(below, False)

        @pl.when(at == steps - 1)
        def _():
            edge(above, True)

    return kernel


def fine_levels(place, below, here, above, slots, stride):
    sizes = []
    for level in range(2):
        period = GRID >> level
        sizes.append(
            (
                (ROWS >> level) // lax.axis_size("brick"),
                period // lax.axis_size(COLUMNS),
                period,
            )
        )
    planes = max(HALF * sizes[0][1], sizes[0][0] * SIDE, sizes[1][0] * sizes[1][1])
    table_spec = pl.BlockSpec(here.shape, lambda i: (0, 0))
    return pl.pallas_call(
        fine_kernel(sizes, slots, stride),
        name="fine",
        grid=(sizes[0][0] // HALF,),
        in_specs=[pl.BlockSpec(memory_space=pltpu.SMEM), table_spec, table_spec, table_spec],
        out_specs=[
            pl.BlockSpec((HALF,) + sizes[0][1:], lambda i: (i, 0, 0)),
            pl.BlockSpec(sizes[1], lambda i: (0, 0, 0)),
        ],
        out_shape=[jax.ShapeDtypeStruct(size, jnp.float32) for size in sizes],
        scratch_shapes=[
            pltpu.VMEM((GRID, slots), jnp.bfloat16),
            pltpu.VMEM((GRID, slots), jnp.bfloat16),
            pltpu.VMEM((sizes[0][1], slots), jnp.float32),
            pltpu.VMEM((sizes[0][1], slots), jnp.float32),
            pltpu.VMEM((planes, slots), jnp.bfloat16),
            pltpu.VMEM((2, sizes[0][0], SIDE, GRID), jnp.float32),
        ],
        compiler_params=pltpu.CompilerParams(dimension_semantics=("arbitrary",)),
    )(place, below, here, above)


def wide_levels(place, table):
    bricks = lax.axis_size("brick")
    slots = table.shape[1]
    chunk = math.gcd(slots, 1024)
    shapes = []
    for level in range(2, 5):
        period = GRID >> level
        shapes.append((ROWS >> level, period // bricks, period))

    def kernel(place, values, *refs):
        outs, (depth, lhs) = refs[:3], refs[3:]

        @pl.when(pl.program_id(0) == 0)
        def _():
            for out in outs:
                out[...] = jnp.zeros(out.shape, jnp.float32)

        def whole(row):
            return values[row : row + 1, :]

        def read(lane, lanes):
            return lambda row: values[row : row + 1, lane : lane + lanes]

        fill_depth(depth, read, chunk, GRID >> 2)
        for level, (rows, cols, period), out in zip(range(2, 5), shapes, outs):
            row_values = row_window(0, rows, whole, level)
            col_values = window(place[0] * cols, max(cols, 8), whole, 1, period)
            for c in range(cols):
                lhs[c * rows : (c + 1) * rows, :] = (
                    row_values * col_values[c : c + 1, :]
                ).astype(jnp.bfloat16)
            part = product(lhs[0 : cols * rows, :], depth[0:period, :])
            for c in range(cols):
                out[:, c * period : (c + 1) * period] += part[c * rows : (c + 1) * rows, :]

    return pl.pallas_call(
        kernel,
        name="wide",
        grid=(slots // chunk,),
        in_specs=[
            pl.BlockSpec(memory_space=pltpu.SMEM),
            pl.BlockSpec((table.shape[0], chunk), lambda i: (0, i)),
        ],
        out_specs=[pl.BlockSpec((r, c * p), lambda i: (0, 0)) for r, c, p in shapes],
        out_shape=[jax.ShapeDtypeStruct((r, c * p), jnp.float32) for r, c, p in shapes],
        scratch_shapes=[
            pltpu.VMEM((GRID >> 2, chunk), jnp.bfloat16),
            pltpu.VMEM((shapes[0][0] * shapes[0][1], chunk), jnp.bfloat16),
        ],
        compiler_params=pltpu.CompilerParams(dimension_semantics=("arbitrary",)),
    )(place, table)


def per_device(
    fine_cells,
    fine_exponent,
    fine_charge,
    fine_offset,
    wide_cells,
    wide_exponent,
    wide_charge,
    wide_offset,
):
    place = jnp.stack([lax.axis_index("brick"), lax.axis_index(COLUMNS)]).astype(jnp.int32)
    slots = fine_exponent.shape[0]
    stride = slots + wide_exponent.shape[0]
    mine = jnp.concatenate(
        [
            pack(fine_cells, fine_exponent, fine_charge, fine_offset),
            pack(wide_cells, wide_exponent, wide_charge, wide_offset),
        ],
        1,
    )

    def wides(block):
        near = [block[:, b * stride + slots : (b + 1) * stride] for b in range(3)]
        return near + [block[:, 3 * stride :]]

    left = shifted(mine, COLUMNS, 1)
    right = shifted(mine, COLUMNS, -1)
    others = [
        shifted(mine[:, slots:], COLUMNS, by) for by in range(2, lax.axis_size(COLUMNS) - 1)
    ]
    here = jnp.concatenate([left, mine, right] + others, 1)
    below = shifted(here, "brick", 1)
    above = shifted(here, "brick", -1)
    column = jnp.concatenate(wides(here), 1)
    far = [shifted(column, "brick", by) for by in range(2, lax.axis_size("brick") - 1)]
    wide = jnp.concatenate([column] + wides(below) + wides(above) + far, 1)
    coarse = wide_levels(place, wide)
    first, second = fine_levels(place, below, here, above, slots, stride)
    return (first, second, coarse[0], coarse[1], coarse[2])


def solution(mesh):
    slots = ("parts", "brick", "rep", "sub")
    return jax.shard_map(
        per_device,
        mesh=mesh,
        in_specs=(
            P(None, slots),
            P(slots),
            P(slots),
            P(None, slots),
            P(None, slots),
            P(slots),
            P(slots),
            P(None, slots),
        ),
        out_specs=(
            P(("parts", "brick"), COLUMNS, None),
            P(("parts", "brick"), COLUMNS, None),
            P("parts", "brick"),
            P("parts", "brick"),
            P("parts", "brick"),
        ),
        check_vma=False,
    )
```
